32 devices in a mesh: ep: 8 (over y, x, core), dp: 4 (over z).
Axes of the slice: x: 2, y: 2, z: 4, core: 2. Of those that a mesh axis runs over, the one named last changes fastest.
Arguments:
- tokens: bfloat16 [4096, 1792], P(('ep', 'dp')), may hold values from -6 to 6
- cotangent: bfloat16 [4096, 1792], P(('ep', 'dp')), may hold values from -6 to 6
- slot_choice: int32 [4096, 2], P(('ep', 'dp')), may hold values from 0 to 7, all different within a row; in each aligned block of 128 rows (0 to 127, 128 to 255, ...) at most 40 rows name the same one
- gate_values: float32 [4096, 2], P(('ep', 'dp')), may hold values from 0.1 to 1
- slot_expert: int32 [8], replicated, may hold values from 0 to 3, as said below
- gate_weight: bfloat16 [8, 1792, 1280], P('ep', None, 'dp'), as said below
- up_weight: bfloat16 [8, 1792, 1280], P('ep', None, 'dp'), as said below
- down_weight: bfloat16 [8, 1280, 1792], P('ep', 'dp'), as said below
Outputs:
- token_grad: bfloat16 [4096, 1792], P(('ep', 'dp'))
- down_grad: bfloat16 [8, 1280, 1792], P('ep', 'dp')
The draws below stay inside these ranges and needn't reach their ends.
Inputs may be any that keep to these rules, and one draw needn't show every extreme that they name: `slot_choice`: each row names 2 different slots; among the rows of one device no slot is named more than 40 times, a bound that some block reaches. `slot_expert`: every expert is held by at least one slot. `gate_weight`: slots that hold the same expert have equal matrices. `up_weight`: slots that hold the same expert have equal matrices. `down_weight`: slots that hold the same expert have equal matrices.
All inputs are finite; a program needn't handle non-finite values.
Results may differ from the reference program's by a relative error of at most 0.0098.
Values may be sent and summed in bfloat16 or wider, within the bound.
A program may use at most 128 MiB of HBM per device.

```python
import math
import jax
import jax.numpy as jnp
import numpy as np
from jax import lax

D = 1792
FF = 1280
TOPK = 2
TOK_DEV = 128
SLOTS = 8
EXPERTS = 4
CAP = 40
TOKENS = 4096


def holder_table(key):
    primary = jnp.arange(EXPERTS, dtype=jnp.int32)
    extra = jax.random.randint(jax.random.fold_in(key, 101), (SLOTS - EXPERTS,), 0, EXPERTS, dtype=jnp.int32)
    order = jax.random.permutation(jax.random.fold_in(key, 102), SLOTS)
    return jnp.concatenate([primary, extra])[order]


def expert_matrices(key, salt, shape, fan):
    base = jax.random.normal(jax.random.fold_in(key, salt), shape, jnp.float32) * fan ** (-0.5)
    return base[holder_table(key)].astype(jnp.bfloat16)


def draw_slot_expert(key, part):
    return holder_table(key)


def draw_gate_weight(key, part):
    return expert_matrices(key, 201, (EXPERTS, D, FF), D)


def draw_up_weight(key, part):
    return expert_matrices(key, 202, (EXPERTS, D, FF), D)


def draw_down_weight(key, part):
    return expert_matrices(key, 203, (EXPERTS, FF, D), FF)


def levels(rng, extent, cuts, smallest, largest):
    level = 1.0
    for dim, parts in cuts:
        heights = jax.random.uniform(jax.random.fold_in(jax.random.fold_in(rng, 6), dim), (parts,), jnp.float32, smallest / len(cuts), largest / len(cuts))
        level = level * jnp.repeat(jnp.exp(heights), extent[dim] // parts).reshape((-1,) + (1,) * (len(extent) - 1 - dim))
    return level


def shared_out(stream_key, own, number, rows, number_of, top, limit, lean):
    order = jax.random.permutation(stream_key, number_of)
    heavy_load, usual = shares(number_of, rows * top, limit, lean, True), shares(number_of, rows * top, limit, lean, False)
    places = jnp.arange(number_of)

    def named(lengths, rotation):
        used = int((lengths > 0).sum())
        fixed = max(1, used // 4)
        moved = fixed + (places - fixed + rotation * (used - fixed)) % max(1, number_of - fixed)
        return jnp.zeros((number_of,), jnp.int32).at[order[jnp.where(places < fixed, places, moved)]].set(jnp.asarray(lengths, jnp.int32))

    lengths = jnp.where(number % 4 == 0, named(heavy_load, number // 4), named(usual, number - number // 4 - 1))
    mixed = jax.random.permutation(jax.random.fold_in(own, 3), number_of)
    source_of, receiver = mixed[0:number_of // 2 * 2:2], mixed[1:number_of // 2 * 2:2]
    margin = jnp.minimum(lengths[source_of] - 1, limit - lengths[receiver]) // 2
    margin = jnp.where((source_of == order[0]) | (receiver == order[0]) | (lengths[receiver] == 0), 0, jnp.maximum(margin, 0))
    moved = jax.random.randint(jax.random.fold_in(own, 4), (number_of // 2,), 0, 1 << 20) % (margin + 1)
    lengths = lengths.at[source_of].add(-moved).at[receiver].add(moved)
    items = jnp.searchsorted(jnp.cumsum(lengths), jnp.arange(rows * top), side="right").astype(jnp.int32)
    grid = items.reshape(top, rows).T
    grid = grid[jax.random.permutation(jax.random.fold_in(own, 1), rows)]
    rotation = jax.random.randint(jax.random.fold_in(own, 2), (rows, 1), 0, top)
    return jnp.take_along_axis(grid, (jnp.arange(top)[None, :] + rotation) % top, axis=1)


def shares(count, total, most, skew, full):
    portions = [(1 << 20) // math.isqrt(grade ** skew) + 1 for grade in range(1, count + 1)]
    largest = most if full else min(most, max(-(-total // count), total * portions[0] // sum(portions)))
    least = 1 if total - largest >= count - 1 else 0
    holding, rest = [largest] + [least] * (count - 1), total - largest - least * (count - 1)
    while rest > 0:
        free = [i for i in range(1, count) if holding[i] < largest] or [i for i in range(1, count) if holding[i] < most]
        pool, budget = sum([portions[i] for i in free]), rest
        for i in free:
            more = min(most - holding[i], max(1, budget * portions[i] // pool), rest)
            holding[i] = holding[i] + more
            rest = rest - more
    return np.array(holding)


def gaussian(stream_key, extent, spread, most, shards=(), held_as=jnp.bfloat16):
    level = levels(stream_key, extent, shards, -0.22, 0.18) if shards else 1.0
    entries = jax.random.normal(stream_key, extent, jnp.float32) * spread * level
    return jnp.minimum(jnp.maximum(entries, -most), most).astype(held_as)


def setup_inputs(seed: int = 0) -> dict:
    streams_of = jax.random.split(jax.random.key(seed), 9)
    tokens = gaussian(streams_of[0], (TOKENS, D), 1.0, 6.0, ((0, 32),))
    cotangent = gaussian(streams_of[1], (TOKENS, D), 1.0, 6.0, ((0, 32),))
    slot_choice_keys = jax.random.split(jax.random.fold_in(streams_of[2], 1), TOKENS // TOK_DEV)
    slot_choice_turns = jax.random.permutation(jax.random.fold_in(streams_of[2], 3), TOKENS // TOK_DEV)
    slot_choice = jax.vmap(lambda own, number: shared_out(jax.random.fold_in(streams_of[2], 2), own, number, TOK_DEV, SLOTS, TOPK, CAP, 2))(slot_choice_keys, slot_choice_turns).reshape((TOKENS, TOPK))
    gate_values = jnp.clip(jnp.exp(math.log(1.0) - 2.3025851 * jax.random.uniform(streams_of[3], (TOKENS, TOPK), jnp.float32) ** levels(streams_of[3], (TOKENS, TOPK), ((0, 32),), -0.2, 0.2)), 0.1, 1.0)
    slot_expert = draw_slot_expert(jax.random.fold_in(streams_of[8], 71), 0)
    gate_weight = draw_gate_weight(jax.random.fold_in(streams_of[8], 71), 0)
    up_weight = draw_up_weight(jax.random.fold_in(streams_of[8], 71), 0)
    down_weight = draw_down_weight(jax.random.fold_in(streams_of[8], 71), 0)
    return dict(tokens=tokens, cotangent=cotangent, slot_choice=slot_choice, gate_values=gate_values, slot_expert=slot_expert, gate_weight=gate_weight, up_weight=up_weight, down_weight=down_weight)


def slot_backward(operands):
    rows_x, rows_g, w_gate, w_up, w_down = operands
    gate = jnp.dot(rows_x, w_gate, preferred_element_type=jnp.float32)
    up = jnp.dot(rows_x, w_up, preferred_element_type=jnp.float32)
    sig = jax.nn.sigmoid(gate)
    act = (gate * sig * up).astype(jnp.bfloat16)
    d_act = jnp.dot(rows_g, w_down.T, preferred_element_type=jnp.float32)
    d_gate = (d_act * up * sig * (1.0 + gate * (1.0 - sig))).astype(jnp.bfloat16)
    d_up = (d_act * gate * sig).astype(jnp.bfloat16)
    contrib = jnp.dot(d_gate, w_gate.T, preferred_element_type=jnp.float32)
    contrib = contrib + jnp.dot(d_up, w_up.T, preferred_element_type=jnp.float32)
    grad = jnp.dot(act.T, rows_g, preferred_element_type=jnp.float32)
    return contrib.astype(jnp.bfloat16), grad


def reference(tokens, cotangent, slot_choice, gate_values, slot_expert, gate_weight, up_weight, down_weight):
    blocks = TOKENS // TOK_DEV
    items = TOK_DEV * TOPK
    choice_b = slot_choice.reshape(blocks, items).astype(jnp.int32)
    onehot = (choice_b[:, :, None] == jnp.arange(SLOTS, dtype=jnp.int32)[None, None, :]).astype(jnp.int32)
    position = jnp.sum(jnp.cumsum(onehot, axis=1) * onehot, axis=2) - 1
    block_id = jnp.arange(blocks, dtype=jnp.int32)[:, None]
    dest = (choice_b * (blocks * CAP) + block_id * CAP + position).reshape(-1).astype(jnp.int32)
    total_rows = SLOTS * blocks * CAP
    source = jnp.full((total_rows,), TOKENS * TOPK, jnp.int32)
    source = source.at[dest].set(jnp.arange(TOKENS * TOPK, dtype=jnp.int32))
    zero_row = jnp.zeros((1, D), jnp.bfloat16)
    item_x = jnp.concatenate([jnp.repeat(tokens, TOPK, axis=0), zero_row], axis=0)
    scaled = cotangent.astype(jnp.float32)[:, None, :] * gate_values.astype(jnp.float32)[:, :, None]
    scaled = scaled.reshape(TOKENS * TOPK, D).astype(jnp.bfloat16)
    item_g = jnp.concatenate([scaled, zero_row], axis=0)
    rows_x = item_x[source].reshape(SLOTS, blocks * CAP, D)
    rows_g = item_g[source].reshape(SLOTS, blocks * CAP, D)
    contrib, grads = lax.map(slot_backward, (rows_x, rows_g, gate_weight, up_weight, down_weight))
    picked = contrib.reshape(total_rows, D)[dest].astype(jnp.float32).reshape(TOKENS, TOPK, D)
    token_grad = jnp.sum(picked, axis=1).astype(jnp.bfloat16)
    same = (slot_expert[:, None] == slot_expert[None, :]).astype(jnp.float32)
    summed = jnp.einsum("st,tfd->sfd", same, grads, precision=lax.Precision.HIGHEST)
    return token_grad, summed.astype(jnp.bfloat16)
```

```python
import functools

import jax
import jax.numpy as jnp
from jax import lax
from jax.experimental import pallas as pl
from jax.experimental.pallas import tpu as pltpu
from jax.sharding import PartitionSpec as P

MESH = pl.DeviceIdType.MESH
VMEM_LIMIT = 60 * 1024 * 1024


def greet(n_ep, n_dp, ep, dp):
    barrier = pltpu.get_barrier_semaphore()

    def greet_ep(k, _):
        peer = lax.rem(ep + k + 1, n_ep)
        pl.semaphore_signal(barrier, inc=1, device_id=(peer, dp), device_id_type=MESH)
        return 0

    lax.fori_loop(0, n_ep - 1, greet_ep, 0)
    for t in range(1, n_dp):
        pl.semaphore_signal(
            barrier, inc=1, device_id=(ep, lax.rem(dp + t, n_dp)), device_id_type=MESH
        )
    pl.semaphore_wait(barrier, n_ep + n_dp - 2)


def dispatch_kernel(
    n_ep, n_dp, cap, topk,
    x_ref, c_ref, meta_ref,
    out_x, out_g, meta_out,
    xbuf, cbuf, mbuf, sx, sg,
    zsend, zrecv, esend, erecv, local,
):
    ep, dp = lax.axis_index("ep"), lax.axis_index("dp")
    tok = x_ref.shape[0]
    greet(n_ep, n_dp, ep, dp)

    def along(t):
        target = (ep, lax.rem(dp + n_dp - t, n_dp))
        pairs = ((meta_ref, mbuf), (x_ref, xbuf), (c_ref, cbuf))
        return [
            pltpu.make_async_remote_copy(
                src_ref=src,
                dst_ref=dst.at[t - 1],
                send_sem=zsend.at[t - 1, i],
                recv_sem=zrecv.at[t - 1, i],
                device_id=target,
                device_id_type=MESH,
            )
            for i, (src, dst) in enumerate(pairs)
        ]

    def across(t, k):
        slot = lax.rem(ep + k + 1, n_ep)
        group = lax.rem(dp + t, n_dp)
        return [
            pltpu.make_async_remote_copy(
                src_ref=src.at[t, slot],
                dst_ref=dst.at[group, ep],
                send_sem=esend.at[i, t, k],
                recv_sem=erecv.at[i, t, k],
                device_id=(slot, dp),
                device_id_type=MESH,
            )
            for i, (src, dst) in enumerate(((sx, out_x), (sg, out_g)))
        ]

    def keep(t):
        group = lax.rem(dp + t, n_dp)
        return [
            pltpu.make_async_copy(src.at[t, ep], dst.at[group, ep], local.at[i, t])
            for i, (src, dst) in enumerate(((sx, out_x), (sg, out_g)))
        ]

    for t in range(1, n_dp):
        for copy in along(t):
            copy.start()

    def fill(t, slot, x, c, meta):
        row = (lax.broadcasted_iota(jnp.int32, (cap, tok), 0) + slot * cap).astype(jnp.float32)
        hit = jnp.zeros((cap, tok), jnp.float32)
        weight = jnp.zeros((cap, tok), jnp.float32)
        for k in range(topk):
            same = meta[k : k + 1, :] == row
            hit = jnp.where(same, 1.0, hit)
            weight = jnp.where(same, meta[topk + k : topk + k + 1, :], weight)
        select = hit.astype(jnp.bfloat16)
        weight = jnp.sum(weight, axis=1, keepdims=True)
        sx[t, slot] = jnp.dot(select, x[...], preferred_element_type=jnp.float32).astype(
            jnp.bfloat16
        )
        sg[t, slot] = (
            jnp.dot(select, c[...], preferred_element_type=jnp.float32) * weight
        ).astype(jnp.bfloat16)

    for t in range(n_dp):
        if t == 0:
            x, c, meta_at = x_ref, c_ref, meta_ref
        else:
            for copy in along(t):
                copy.wait_recv()
            x, c, meta_at = xbuf.at[t - 1], cbuf.at[t - 1], mbuf.at[t - 1]
        meta = meta_at[...]
        meta_out[t] = meta

        def step(k, _):
            fill(t, lax.rem(ep + k + 1, n_ep), x, c, meta)
            for copy in across(t, k):
                copy.start()
            return 0

        lax.fori_loop(0, n_ep - 1, step, 0)
        fill(t, ep, x, c, meta)
        for copy in keep(t):
            copy.start()

    for t in range(n_dp):
        def finish(k, _):
            for copy in across(t, k):
                copy.wait_recv()
                copy.wait_send()
            return 0

        lax.fori_loop(0, n_ep - 1, finish, 0)
        for copy in keep(t):
            copy.wait()
        if t > 0:
            for copy in along(t):
                copy.wait_send()


def combine_kernel(
    n_ep, n_dp, cap, topk,
    part, pieces, dest, expert,
    token_out, grad_out,
    back, gbuf, cbuf, zout, zin, total,
    gsend, grecv, csend, crecv, bsend, brecv, zsend, zrecv, local,
):
    ep, dp = lax.axis_index("ep"), lax.axis_index("dp")
    tok = token_out.shape[0]
    rows, width = pieces.shape[1], pieces.shape[2]
    greet(n_ep, n_dp, ep, dp)

    def give(k):
        peer = lax.rem(ep + k + 1, n_ep)
        return pltpu.make_async_remote_copy(
            src_ref=pieces.at[peer],
            dst_ref=gbuf.at[ep],
            send_sem=gsend.at[k],
            recv_sem=grecv.at[k],
            device_id=(peer, dp),
            device_id_type=MESH,
        )

    def hand_back(k):
        peer = lax.rem(ep + k + 1, n_ep)
        return pltpu.make_async_remote_copy(
            src_ref=cbuf.at[peer],
            dst_ref=grad_out.at[ep],
            send_sem=csend.at[k],
            recv_sem=crecv.at[k],
            device_id=(peer, dp),
            device_id_type=MESH,
        )

    def home(t, k):
        peer = lax.rem(ep + k + 1, n_ep)
        return pltpu.make_async_remote_copy(
            src_ref=part.at[lax.rem(dp + t, n_dp), peer],
            dst_ref=back.at[t, ep],
            send_sem=bsend.at[t, k],
            recv_sem=brecv.at[t, k],
            device_id=(peer, dp),
            device_id_type=MESH,
        )

    def along(t):
        return pltpu.make_async_remote_copy(
            src_ref=zout.at[t - 1],
            dst_ref=zin.at[t - 1],
            send_sem=zsend.at[t - 1],
            recv_sem=zrecv.at[t - 1],
            device_id=(ep, lax.rem(dp + t, n_dp)),
            device_id_type=MESH,
        )

    def loop(fn):
        def body(k, _):
            fn(k)
            return 0

        lax.fori_loop(0, n_ep - 1, body, 0)

    order = list(range(1, n_dp)) + [0]
    loop(lambda k: give(k).start())
    for t in order:
        loop(lambda k: home(t, k).start())

    loop(lambda k: give(k).wait_recv())
    gbuf[ep] = pieces[ep]

    def merge(s, _):
        def add(r, acc):
            factor = jnp.where(expert[s] == expert[r], 1.0, 0.0)
            return acc + gbuf[r].astype(jnp.float32) * factor

        acc = lax.fori_loop(0, n_ep, add, jnp.zeros((rows, width), jnp.float32))
        cbuf[s] = acc.astype(jnp.bfloat16)
        return 0

    lax.fori_loop(0, n_ep, merge, 0)
    loop(lambda k: hand_back(k).start())
    own = pltpu.make_async_copy(cbuf.at[ep], grad_out.at[ep], local)
    own.start()

    for t in order:
        loop(lambda k: home(t, k).wait_recv())
        back[t, ep] = part[lax.rem(dp + t, n_dp), ep]
        total[...] = jnp.zeros_like(total)

        def gather(s, _):
            column = (lax.broadcasted_iota(jnp.int32, (tok, cap), 1) + s * cap).astype(jnp.float32)
            hit = jnp.zeros((tok, cap), jnp.float32)
            for k in range(topk):
                hit = jnp.where(dest[t, :, k : k + 1] == column, 1.0, hit)
            total[...] += jnp.dot(
                hit.astype(jnp.bfloat16), back[t, s], preferred_element_type=jnp.float32
            )
            return 0

        lax.fori_loop(0, n_ep, gather, 0)
        if t > 0:
            zout[t - 1] = total[...].astype(jnp.bfloat16)
            along(t).start()

    for t in range(1, n_dp):
        along(t).wait_recv()
        total[...] += zin[t - 1].astype(jnp.float32)
    token_out[...] = total[...].astype(token_out.dtype)

    loop(lambda k: give(k).wait_send())
    loop(lambda k: hand_back(k).wait())
    for t in range(n_dp):
        loop(lambda k: home(t, k).wait_send())
    for t in range(1, n_dp):
        along(t).wait_send()
    own.wait()


def per_device(
    tokens, cotangent, slot_choice, gate_values, slot_expert, gate_weight, up_weight, down_weight
):
    n_ep, n_dp = lax.axis_size("ep"), lax.axis_size("dp")
    tok, width = tokens.shape
    topk = slot_choice.shape[1]
    cap = max(2, 5 * tok * topk // (4 * n_ep))
    flat_slot = slot_choice.reshape(-1)
    onehot = (flat_slot[:, None] == jnp.arange(n_ep, dtype=jnp.int32)[None, :]).astype(jnp.int32)
    position = jnp.sum(jnp.cumsum(onehot, axis=0) * onehot, axis=1) - 1
    dest = (flat_slot * cap + position).reshape(tok, topk)
    lines = -(-2 * topk // 8) * 8
    meta = jnp.concatenate(
        [
            dest.T.astype(jnp.float32),
            gate_values.T,
            jnp.zeros((lines - 2 * topk, tok), jnp.float32),
        ],
        axis=0,
    )
    vmem = pl.BlockSpec(memory_space=pltpu.VMEM)
    anywhere = pl.BlockSpec(memory_space=pl.ANY)
    dma = pltpu.SemaphoreType.DMA
    bf16 = jnp.bfloat16
    routed = jax.ShapeDtypeStruct((n_dp, n_ep, cap, width), bf16)
    rows_x, rows_g, meta_all = pl.pallas_call(
        functools.partial(dispatch_kernel, n_ep, n_dp, cap, topk),
        out_shape=(routed, routed, jax.ShapeDtypeStruct((n_dp, lines, tok), jnp.float32)),
        in_specs=[vmem] * 3,
        out_specs=(anywhere, anywhere, vmem),
        scratch_shapes=[
            pltpu.VMEM((n_dp - 1, tok, width), bf16),
            pltpu.VMEM((n_dp - 1, tok, width), bf16),
            pltpu.VMEM((n_dp - 1, lines, tok), jnp.float32),
            pltpu.VMEM((n_dp, n_ep, cap, width), bf16),
            pltpu.VMEM((n_dp, n_ep, cap, width), bf16),
            dma((n_dp - 1, 3)),
            dma((n_dp - 1, 3)),
            dma((2, n_dp, n_ep)),
            dma((2, n_dp, n_ep)),
            dma((2, n_dp)),
        ],
        compiler_params=pltpu.CompilerParams(
            collective_id=0, has_side_effects=True, vmem_limit_bytes=VMEM_LIMIT
        ),
        name="dispatch",
    )(tokens, cotangent, meta)

    rows_x = rows_x.reshape(-1, width)
    rows_g = rows_g.reshape(-1, width)
    w_gate, w_up, w_down = gate_weight[0], up_weight[0], down_weight[0]
    gate = jnp.dot(rows_x, w_gate, preferred_element_type=jnp.float32)
    up = jnp.dot(rows_x, w_up, preferred_element_type=jnp.float32)
    sig = jax.nn.sigmoid(gate)
    act = (gate * sig * up).astype(bf16)
    d_act = lax.dot_general(
        rows_g, w_down, (((1,), (1,)), ((), ())), preferred_element_type=jnp.float32
    )
    d_gate = (d_act * up * sig * (1.0 + gate * (1.0 - sig))).astype(bf16)
    d_up = (d_act * gate * sig).astype(bf16)
    part = lax.dot_general(
        d_gate, w_gate, (((1,), (1,)), ((), ())), preferred_element_type=jnp.float32
    )
    part = part + lax.dot_general(
        d_up, w_up, (((1,), (1,)), ((), ())), preferred_element_type=jnp.float32
    )
    part = part.astype(bf16).reshape(n_dp, n_ep, cap, width)
    slot_grad = lax.dot_general(
        act, rows_g, (((0,), (0,)), ((), ())), preferred_element_type=jnp.float32
    )
    hidden = slot_grad.shape[0]
    piece = hidden // n_ep
    pieces = slot_grad.astype(bf16).reshape(n_ep, piece, width)

    token_grad, down_grad = pl.pallas_call(
        functools.partial(combine_kernel, n_ep, n_dp, cap, topk),
        out_shape=(
            jax.ShapeDtypeStruct((tok, width), bf16),
            jax.ShapeDtypeStruct((n_ep, piece, width), bf16),
        ),
        in_specs=[vmem, vmem, vmem, pl.BlockSpec(memory_space=pltpu.SMEM)],
        out_specs=(vmem, anywhere),
        scratch_shapes=[
            pltpu.VMEM((n_dp, n_ep, cap, width), bf16),
            pltpu.VMEM((n_ep, piece, width), bf16),
            pltpu.VMEM((n_ep, piece, width), bf16),
            pltpu.VMEM((n_dp - 1, tok, width), bf16),
            pltpu.VMEM((n_dp - 1, tok, width), bf16),
            pltpu.VMEM((tok, width), jnp.float32),
            dma((n_ep,)),
            dma((n_ep,)),
            dma((n_ep,)),
            dma((n_ep,)),
            dma((n_dp, n_ep)),
            dma((n_dp, n_ep)),
            dma((n_dp - 1,)),
            dma((n_dp - 1,)),
            dma,
        ],
        compiler_params=pltpu.CompilerParams(
            collective_id=1, has_side_effects=True, vmem_limit_bytes=VMEM_LIMIT
        ),
        name="combine",
    )(part, pieces, jnp.swapaxes(meta_all[:, :topk, :], 1, 2), slot_expert)
    return token_grad, down_grad.reshape(1, hidden, width)


def solution(mesh):
    return jax.shard_map(
        per_device,
        mesh=mesh,
        in_specs=(
            P(("ep", "dp"), None),
            P(("ep", "dp"), None),
            P(("ep", "dp"), None),
            P(("ep", "dp"), None),
            P(),
            P("ep", None, "dp"),
            P("ep", None, "dp"),
            P("ep", "dp", None),
        ),
        out_specs=(P(("ep", "dp"), None), P("ep", "dp", None)),
        check_vma=False,
    )
```

```python
import functools

import jax
import jax.numpy as jnp
from jax import lax
from jax.experimental import pallas as pl
from jax.experimental.pallas import tpu as pltpu
from jax.sharding import PartitionSpec as P

MESH = pl.DeviceIdType.MESH
VMEM_LIMIT = 60 * 1024 * 1024


def greet(n_ep, n_dp, ep, dp):
    barrier = pltpu.get_barrier_semaphore()

    def greet_ep(k, _):
        peer = lax.rem(ep + k + 1, n_ep)
        pl.semaphore_signal(barrier, inc=1, device_id=(peer, dp), device_id_type=MESH)
        return 0

    lax.fori_loop(0, n_ep - 1, greet_ep, 0)
    for t in range(1, n_dp):
        pl.semaphore_signal(
            barrier, inc=1, device_id=(ep, lax.rem(dp + t, n_dp)), device_id_type=MESH
        )
    pl.semaphore_wait(barrier, n_ep + n_dp - 2)


def dispatch_kernel(
    n_ep, n_dp, cap, topk, early, batch,
    x_ref, c_ref, meta_ref,
    out_x, out_g, meta_out,
    xbuf, cbuf, mbuf, sx_own, sg_own, sx, sg,
    zsend, zrecv, csend, crecv, esend, erecv, local,
):
    ep, dp = lax.axis_index("ep"), lax.axis_index("dp")
    tok, width = x_ref.shape
    late = width - early
    first, rest = pl.ds(0, early), pl.ds(early, late)
    outs = (out_x, out_g)
    greet(n_ep, n_dp, ep, dp)

    near = [
        sorted(range(n_dp), key=lambda j: (abs(j - z), -j if 2 * z < n_dp else j))
        for z in range(n_dp)
    ]

    def group_of(t):
        return sum(jnp.where(dp == z, near[z][t], 0) for z in range(n_dp))

    groups = [dp] + [group_of(t) for t in range(1, n_dp)]

    def raw(t, way):
        g = groups[t]
        if t == 0:
            srcs = (meta_ref, x_ref.at[:, rest], c_ref.at[:, rest])
        else:
            srcs = (mbuf.at[g], xbuf.at[g], cbuf.at[g])
        return [
            pltpu.make_async_remote_copy(
                src_ref=src,
                dst_ref=dst.at[g],
                send_sem=zsend.at[g, i, way],
                recv_sem=zrecv.at[g, i],
                device_id=(ep, lax.rem(dp + n_dp + 1 - 2 * way, n_dp)),
                device_id_type=MESH,
            )
            for i, (src, dst) in enumerate(zip(srcs, (mbuf, xbuf, cbuf)))
        ]

    def columns(t, way):
        g = groups[t]
        return [
            pltpu.make_async_remote_copy(
                src_ref=out.at[g, :, :, first],
                dst_ref=out.at[g, :, :, first],
                send_sem=csend.at[g, i, way],
                recv_sem=crecv.at[g, i],
                device_id=(ep, lax.rem(dp + n_dp + 1 - 2 * way, n_dp)),
                device_id_type=MESH,
            )
            for i, out in enumerate(outs)
        ]

    def pass_on(make, t, act):
        g = groups[t]

        @pl.when((g <= dp) & (dp < n_dp - 1))
        def _():
            for copy in make(t, 0):
                act(copy)

        @pl.when((g >= dp) & (dp > 0))
        def _():
            for copy in make(t, 1):
                act(copy)

    def start(copy):
        copy.start()

    def wait_send(copy):
        copy.wait_send()

    def ends(t, out, at):
        g = groups[t]
        return out.at[g, at] if t == 0 else out.at[g, at, :, rest]

    def made(t):
        return (sx_own, sg_own) if t == 0 else (sx.at[t - 1], sg.at[t - 1])

    def across(t, slot, source):
        return [
            pltpu.make_async_remote_copy(
                src_ref=src.at[slot],
                dst_ref=ends(t, out, source),
                send_sem=esend.at[i, t, slot],
                recv_sem=erecv.at[i, t, source],
                device_id=(slot, dp),
                device_id_type=MESH,
            )
            for i, (src, out) in enumerate(zip(made(t), outs))
        ]

    def keep(t):
        return [
            pltpu.make_async_copy(src.at[ep], ends(t, out, ep), local.at[i, t])
            for i, (src, out) in enumerate(zip(made(t), outs))
        ]

    def others(fn):
        def body(k, _):
            fn(lax.rem(ep + k + 1, n_ep))
            return 0

        lax.fori_loop(0, n_ep - 1, body, 0)

    def arrived(t):
        def body(peer):
            for copy in across(t, peer, peer):
                copy.wait_recv()

        others(body)
        for copy in keep(t):
            copy.wait()

    def fill(t, base, x, c, meta):
        shape = (batch * cap, tok)
        row = (lax.broadcasted_iota(jnp.int32, shape, 0) + base * cap).astype(jnp.float32)
        hit = jnp.zeros(shape, jnp.float32)
        weight = jnp.zeros(shape, jnp.float32)
        for k in range(topk):
            same = meta[k : k + 1, :] == row
            hit = jnp.where(same, 1.0, hit)
            weight = jnp.where(same, meta[topk + k : topk + k + 1, :], weight)
        select = hit.astype(jnp.bfloat16)
        weight = jnp.sum(weight, axis=1, keepdims=True)
        to_x, to_g = made(t)
        rows = jnp.dot(select, x[...], preferred_element_type=jnp.float32)
        for i in range(batch):
            to_x[base + i] = rows[i * cap : (i + 1) * cap].astype(jnp.bfloat16)
        rows = jnp.dot(select, c[...], preferred_element_type=jnp.float32) * weight
        for i in range(batch):
            to_g[base + i] = rows[i * cap : (i + 1) * cap].astype(jnp.bfloat16)

    pass_on(raw, 0, start)
    for t in range(n_dp):
        if t == 0:
            x, c, meta_at = x_ref, c_ref, meta_ref
        else:
            for copy in raw(t, 0):
                copy.wait_recv()
            pass_on(raw, t, start)
            g = groups[t]
            x, c, meta_at = xbuf.at[g], cbuf.at[g], mbuf.at[g]
        meta = meta_at[...]
        meta_out[groups[t]] = meta

        def step(k, _):
            base = lax.rem((ep // batch + k + 1) * batch, n_ep)
            fill(t, base, x, c, meta)
            for i in range(batch):
                slot = base + lax.rem(ep + i, batch)

                @pl.when(slot != ep)
                def _():
                    for copy in across(t, slot, ep):
                        copy.start()

            return 0

        lax.fori_loop(0, n_ep // batch, step, 0)
        for copy in keep(t):
            copy.start()
        if t == min(2, n_dp - 1):
            arrived(0)
            pass_on(columns, 0, start)

    for t in range(1, n_dp):
        for copy in columns(t, 0):
            copy.wait_recv()
        pass_on(columns, t, start)
    for t in range(1, n_dp):
        arrived(t)

    for t in range(n_dp):
        pass_on(raw, t, wait_send)
        pass_on(columns, t, wait_send)

        def sent(peer):
            for copy in across(t, peer, ep):
                copy.wait_send()

        others(sent)


def combine_kernel(
    n_ep, n_dp, cap, topk,
    part, pieces, dest, expert,
    token_out, grad_out,
    back, gbuf, cbuf, zout, zin, total,
    gsend, grecv, csend, crecv, bsend, brecv, zsend, zrecv, local,
):
    ep, dp = lax.axis_index("ep"), lax.axis_index("dp")
    tok = token_out.shape[0]
    rows, width = pieces.shape[1], pieces.shape[2]
    greet(n_ep, n_dp, ep, dp)

    def give(k):
        peer = lax.rem(ep + k + 1, n_ep)
        return pltpu.make_async_remote_copy(
            src_ref=pieces.at[peer],
            dst_ref=gbuf.at[ep],
            send_sem=gsend.at[k],
            recv_sem=grecv.at[k],
            device_id=(peer, dp),
            device_id_type=MESH,
        )

    def hand_back(k):
        peer = lax.rem(ep + k + 1, n_ep)
        return pltpu.make_async_remote_copy(
            src_ref=cbuf.at[peer],
            dst_ref=grad_out.at[ep],
            send_sem=csend.at[k],
            recv_sem=crecv.at[k],
            device_id=(peer, dp),
            device_id_type=MESH,
        )

    def home(t, k):
        peer = lax.rem(ep + k + 1, n_ep)
        return pltpu.make_async_remote_copy(
            src_ref=part.at[lax.rem(dp + t, n_dp), peer],
            dst_ref=back.at[t, ep],
            send_sem=bsend.at[t, k],
            recv_sem=brecv.at[t, k],
            device_id=(peer, dp),
            device_id_type=MESH,
        )

    def along(t):
        return pltpu.make_async_remote_copy(
            src_ref=zout.at[t - 1],
            dst_ref=zin.at[t - 1],
            send_sem=zsend.at[t - 1],
            recv_sem=zrecv.at[t - 1],
            device_id=(ep, lax.rem(dp + t, n_dp)),
            device_id_type=MESH,
        )

    def loop(fn):
        def body(k, _):
            fn(k)
            return 0

        lax.fori_loop(0, n_ep - 1, body, 0)

    order = list(range(1, n_dp)) + [0]
    loop(lambda k: give(k).start())
    for t in order:
        loop(lambda k: home(t, k).start())

    loop(lambda k: give(k).wait_recv())
    gbuf[ep] = pieces[ep]

    def merge(s, _):
        def add(r, acc):
            factor = jnp.where(expert[s] == expert[r], 1.0, 0.0)
            return acc + gbuf[r].astype(jnp.float32) * factor

        acc = lax.fori_loop(0, n_ep, add, jnp.zeros((rows, width), jnp.float32))
        cbuf[s] = acc.astype(jnp.bfloat16)
        return 0

    lax.fori_loop(0, n_ep, merge, 0)
    loop(lambda k: hand_back(k).start())
    own = pltpu.make_async_copy(cbuf.at[ep], grad_out.at[ep], local)
    own.start()

    for t in order:
        loop(lambda k: home(t, k).wait_recv())
        back[t, ep] = part[lax.rem(dp + t, n_dp), ep]
        total[...] = jnp.zeros_like(total)

        def gather(s, _):
            column = (lax.broadcasted_iota(jnp.int32, (tok, cap), 1) + s * cap).astype(jnp.float32)
            hit = jnp.zeros((tok, cap), jnp.float32)
            for k in range(topk):
                hit = jnp.where(dest[lax.rem(dp + t, n_dp), :, k : k + 1] == column, 1.0, hit)
            total[...] += jnp.dot(
                hit.astype(jnp.bfloat16), back[t, s], preferred_element_type=jnp.float32
            )
            return 0

        lax.fori_loop(0, n_ep, gather, 0)
        if t > 0:
            zout[t - 1] = total[...].astype(jnp.bfloat16)
            along(t).start()

    for t in range(1, n_dp):
        along(t).wait_recv()
        total[...] += zin[t - 1].astype(jnp.float32)
    token_out[...] = total[...].astype(token_out.dtype)

    loop(lambda k: give(k).wait_send())
    loop(lambda k: hand_back(k).wait())
    for t in range(n_dp):
        loop(lambda k: home(t, k).wait_send())
    for t in range(1, n_dp):
        along(t).wait_send()
    own.wait()


def per_device(
    tokens, cotangent, slot_choice, gate_values, slot_expert, gate_weight, up_weight, down_weight
):
    n_ep, n_dp = lax.axis_size("ep"), lax.axis_size("dp")
    tok, width = tokens.shape
    topk = slot_choice.shape[1]
    cap = max(2, 5 * tok * topk // (4 * n_ep))
    flat_slot = slot_choice.reshape(-1)
    onehot = (flat_slot[:, None] == jnp.arange(n_ep, dtype=jnp.int32)[None, :]).astype(jnp.int32)
    position = jnp.sum(jnp.cumsum(onehot, axis=0) * onehot, axis=1) - 1
    dest = (flat_slot * cap + position).reshape(tok, topk)
    lines = -(-2 * topk // 8) * 8
    meta = jnp.concatenate(
        [
            dest.T.astype(jnp.float32),
            gate_values.T,
            jnp.zeros((lines - 2 * topk, tok), jnp.float32),
        ],
        axis=0,
    )
    vmem = pl.BlockSpec(memory_space=pltpu.VMEM)
    anywhere = pl.BlockSpec(memory_space=pl.ANY)
    dma = pltpu.SemaphoreType.DMA
    bf16 = jnp.bfloat16
    early = 3 * width // (14 * 128) * 128
    batch = 4 if cap % 8 == 0 and n_ep % 4 == 0 else 1
    routed = jax.ShapeDtypeStruct((n_dp, n_ep, cap, width), bf16)
    rows_x, rows_g, meta_all = pl.pallas_call(
        functools.partial(dispatch_kernel, n_ep, n_dp, cap, topk, early, batch),
        out_shape=(routed, routed, jax.ShapeDtypeStruct((n_dp, lines, tok), jnp.float32)),
        in_specs=[vmem] * 3,
        out_specs=(anywhere, anywhere, vmem),
        scratch_shapes=[
            pltpu.VMEM((n_dp, tok, width - early), bf16),
            pltpu.VMEM((n_dp, tok, width - early), bf16),
            pltpu.VMEM((n_dp, lines, tok), jnp.float32),
            pltpu.VMEM((n_ep, cap, width), bf16),
            pltpu.VMEM((n_ep, cap, width), bf16),
            pltpu.VMEM((n_dp - 1, n_ep, cap, width - early), bf16),
            pltpu.VMEM((n_dp - 1, n_ep, cap, width - early), bf16),
            dma((n_dp, 3, 2)),
            dma((n_dp, 3)),
            dma((n_dp, 2, 2)),
            dma((n_dp, 2)),
            dma((2, n_dp, n_ep)),
            dma((2, n_dp, n_ep)),
            dma((2, n_dp)),
        ],
        compiler_params=pltpu.CompilerParams(
            collective_id=0, has_side_effects=True, vmem_limit_bytes=VMEM_LIMIT
        ),
        name="dispatch",
    )(tokens, cotangent, meta)

    rows_x = rows_x.reshape(-1, width)
    rows_g = rows_g.reshape(-1, width)
    w_gate, w_up, w_down = gate_weight[0], up_weight[0], down_weight[0]
    gate = jnp.dot(rows_x, w_gate, preferred_element_type=jnp.float32)
    up = jnp.dot(rows_x, w_up, preferred_element_type=jnp.float32)
    sig = jax.nn.sigmoid(gate)
    act = (gate * sig * up).astype(bf16)
    d_act = lax.dot_general(
        rows_g, w_down, (((1,), (1,)), ((), ())), preferred_element_type=jnp.float32
    )
    d_gate = (d_act * up * sig * (1.0 + gate * (1.0 - sig))).astype(bf16)
    d_up = (d_act * gate * sig).astype(bf16)
    part = lax.dot_general(
        d_gate, w_gate, (((1,), (1,)), ((), ())), preferred_element_type=jnp.float32
    )
    part = part + lax.dot_general(
        d_up, w_up, (((1,), (1,)), ((), ())), preferred_element_type=jnp.float32
    )
    part = part.astype(bf16).reshape(n_dp, n_ep, cap, width)
    slot_grad = lax.dot_general(
        act, rows_g, (((0,), (0,)), ((), ())), preferred_element_type=jnp.float32
    )
    hidden = slot_grad.shape[0]
    piece = hidden // n_ep
    pieces = slot_grad.astype(bf16).reshape(n_ep, piece, width)

    token_grad, down_grad = pl.pallas_call(
        functools.partial(combine_kernel, n_ep, n_dp, cap, topk),
        out_shape=(
            jax.ShapeDtypeStruct((tok, width), bf16),
            jax.ShapeDtypeStruct((n_ep, piece, width), bf16),
        ),
        in_specs=[vmem, vmem, vmem, pl.BlockSpec(memory_space=pltpu.SMEM)],
        out_specs=(vmem, anywhere),
        scratch_shapes=[
            pltpu.VMEM((n_dp, n_ep, cap, width), bf16),
            pltpu.VMEM((n_ep, piece, width), bf16),
            pltpu.VMEM((n_ep, piece, width), bf16),
            pltpu.VMEM((n_dp - 1, tok, width), bf16),
            pltpu.VMEM((n_dp - 1, tok, width), bf16),
            pltpu.VMEM((tok, width), jnp.float32),
            dma((n_ep,)),
            dma((n_ep,)),
            dma((n_ep,)),
            dma((n_ep,)),
            dma((n_dp, n_ep)),
            dma((n_dp, n_ep)),
            dma((n_dp - 1,)),
            dma((n_dp - 1,)),
            dma,
        ],
        compiler_params=pltpu.CompilerParams(
            collective_id=1, has_side_effects=True, vmem_limit_bytes=VMEM_LIMIT
        ),
        name="combine",
    )(part, pieces, jnp.swapaxes(meta_all[:, :topk, :], 1, 2), slot_expert)
    return token_grad, down_grad.reshape(1, hidden, width)


def solution(mesh):
    return jax.shard_map(
        per_device,
        mesh=mesh,
        in_specs=(
            P(("ep", "dp"), None),
            P(("ep", "dp"), None),
            P(("ep", "dp"), None),
            P(("ep", "dp"), None),
            P(),
            P("ep", None, "dp"),
            P("ep", None, "dp"),
            P("ep", "dp", None),
        ),
        out_specs=(P(("ep", "dp"), None), P("ep", "dp", None)),
        check_vma=False,
    )
```

```python
import functools

import jax
import jax.numpy as jnp
from jax import lax
from jax.experimental import pallas as pl
from jax.experimental.pallas import tpu as pltpu
from jax.sharding import PartitionSpec as P

MESH = pl.DeviceIdType.MESH
VMEM_LIMIT = 60 * 1024 * 1024


def greet(n_ep, n_dp, ep, dp):
    barrier = pltpu.get_barrier_semaphore()

    def greet_ep(k, _):
        peer = lax.rem(ep + k + 1, n_ep)
        pl.semaphore_signal(barrier, inc=1, device_id=(peer, dp), device_id_type=MESH)
        return 0

    lax.fori_loop(0, n_ep - 1, greet_ep, 0)
    for t in range(1, n_dp):
        pl.semaphore_signal(
            barrier, inc=1, device_id=(ep, lax.rem(dp + t, n_dp)), device_id_type=MESH
        )
    pl.semaphore_wait(barrier, n_ep + n_dp - 2)


def dispatch_kernel(
    n_ep, n_dp, cap, topk, early, batch,
    x_ref, c_ref, meta_ref,
    out_x, out_g, meta_out,
    xbuf, cbuf, mbuf, sx_own, sg_own, sx, sg,
    zsend, zrecv, csend, crecv, esend, erecv, local,
):
    ep, dp = lax.axis_index("ep"), lax.axis_index("dp")
    tok, width = x_ref.shape
    late = width - early
    first, rest = pl.ds(0, early), pl.ds(early, late)
    outs = (out_x, out_g)
    greet(n_ep, n_dp, ep, dp)

    near = [
        sorted(range(n_dp), key=lambda j: (abs(j - z), -j if 2 * z < n_dp else j))
        for z in range(n_dp)
    ]

    def group_of(t):
        return sum(jnp.where(dp == z, near[z][t], 0) for z in range(n_dp))

    groups = [dp] + [group_of(t) for t in range(1, n_dp)]

    def raw(t, way):
        g = groups[t]
        if t == 0:
            srcs = (meta_ref, x_ref.at[:, rest], c_ref.at[:, rest])
        else:
            srcs = (mbuf.at[g], xbuf.at[g], cbuf.at[g])
        return [
            pltpu.make_async_remote_copy(
                src_ref=src,
                dst_ref=dst.at[g],
                send_sem=zsend.at[g, i, way],
                recv_sem=zrecv.at[g, i],
                device_id=(ep, lax.rem(dp + n_dp + 1 - 2 * way, n_dp)),
                device_id_type=MESH,
            )
            for i, (src, dst) in enumerate(zip(srcs, (mbuf, xbuf, cbuf)))
        ]

    def columns(t, way):
        g = groups[t]
        return [
            pltpu.make_async_remote_copy(
                src_ref=out.at[g, :, :, first],
                dst_ref=out.at[g, :, :, first],
                send_sem=csend.at[g, i, way],
                recv_sem=crecv.at[g, i],
                device_id=(ep, lax.rem(dp + n_dp + 1 - 2 * way, n_dp)),
                device_id_type=MESH,
            )
            for i, out in enumerate(outs)
        ]

    def pass_on(make, t, act):
        g = groups[t]

        @pl.when((g <= dp) & (dp < n_dp - 1))
        def _():
            for copy in make(t, 0):
                act(copy)

        @pl.when((g >= dp) & (dp > 0))
        def _():
            for copy in make(t, 1):
                act(copy)

    def start(copy):
        copy.start()

    def wait_send(copy):
        copy.wait_send()

    def ends(t, out, at):
        g = groups[t]
        return out.at[g, at] if t == 0 else out.at[g, at, :, rest]

    def made(t):
        return (sx_own, sg_own) if t == 0 else (sx.at[t - 1], sg.at[t - 1])

    def across(t, slot, source):
        return [
            pltpu.make_async_remote_copy(
                src_ref=src.at[slot],
                dst_ref=ends(t, out, source),
                send_sem=esend.at[i, t, slot],
                recv_sem=erecv.at[i, t, source],
                device_id=(slot, dp),
                device_id_type=MESH,
            )
            for i, (src, out) in enumerate(zip(made(t), outs))
        ]

    def keep(t):
        return [
            pltpu.make_async_copy(src.at[ep], ends(t, out, ep), local.at[i, t])
            for i, (src, out) in enumerate(zip(made(t), outs))
        ]

    def others(fn):
        def body(k, _):
            fn(lax.rem(ep + k + 1, n_ep))
            return 0

        lax.fori_loop(0, n_ep - 1, body, 0)

    def arrived(t):
        def body(peer):
            for copy in across(t, peer, peer):
                copy.wait_recv()

        others(body)
        for copy in keep(t):
            copy.wait()

    def fill(t, base, x, c, meta):
        shape = (batch * cap, tok)
        row = (lax.broadcasted_iota(jnp.int32, shape, 0) + base * cap).astype(jnp.float32)
        hit = jnp.zeros(shape, jnp.float32)
        weight = jnp.zeros(shape, jnp.float32)
        for k in range(topk):
            same = meta[k : k + 1, :] == row
            hit = jnp.where(same, 1.0, hit)
            weight = jnp.where(same, meta[topk + k : topk + k + 1, :], weight)
        select = hit.astype(jnp.bfloat16)
        weight = jnp.sum(weight, axis=1, keepdims=True)
        to_x, to_g = made(t)
        rows = jnp.dot(select, x[...], preferred_element_type=jnp.float32)
        for i in range(batch):
            to_x[base + i] = rows[i * cap : (i + 1) * cap].astype(jnp.bfloat16)
        rows = jnp.dot(select, c[...], preferred_element_type=jnp.float32) * weight
        for i in range(batch):
            to_g[base + i] = rows[i * cap : (i + 1) * cap].astype(jnp.bfloat16)

    pass_on(raw, 0, start)
    for t in range(n_dp):
        if t == 0:
            x, c, meta_at = x_ref, c_ref, meta_ref
        else:
            for copy in raw(t, 0):
                copy.wait_recv()
            pass_on(raw, t, start)
            g = groups[t]
            x, c, meta_at = xbuf.at[g], cbuf.at[g], mbuf.at[g]
        meta = meta_at[...]
        meta_out[groups[t]] = meta

        def step(k, _):
            base = lax.rem((ep // batch + k + 1) * batch, n_ep)
            fill(t, base, x, c, meta)
            for i in range(batch):
                slot = base + lax.rem(ep + i, batch)

                @pl.when(slot != ep)
                def _():
                    for copy in across(t, slot, ep):
                        copy.start()

            return 0

        lax.fori_loop(0, n_ep // batch, step, 0)
        for copy in keep(t):
            copy.start()
        if t == min(2, n_dp - 1):
            arrived(0)
            pass_on(columns, 0, start)

    for t in range(1, n_dp):
        for copy in columns(t, 0):
            copy.wait_recv()
        pass_on(columns, t, start)
    for t in range(1, n_dp):
        arrived(t)

    for t in range(n_dp):
        pass_on(raw, t, wait_send)
        pass_on(columns, t, wait_send)

        def sent(peer):
            for copy in across(t, peer, ep):
                copy.wait_send()

        others(sent)


def combine_kernel(
    n_ep, n_dp, cap, topk, early,
    part, pieces, dest, expert,
    token_out, grad_out,
    back, gbuf, cbuf, zout, zin, total, shares, mine,
    gsend, grecv, csend, crecv, bsend, brecv, zsend, zrecv, hsend, hrecv, msend, mrecv, local,
):
    ep, dp = lax.axis_index("ep"), lax.axis_index("dp")
    tok = token_out.shape[0]
    first, rest = pl.ds(0, early), pl.ds(early, pieces.shape[2] - early)
    rows, width = pieces.shape[1], pieces.shape[2]
    greet(n_ep, n_dp, ep, dp)

    def give(k):
        peer = lax.rem(ep + k + 1, n_ep)
        return pltpu.make_async_remote_copy(
            src_ref=pieces.at[peer],
            dst_ref=gbuf.at[ep],
            send_sem=gsend.at[k],
            recv_sem=grecv.at[k],
            device_id=(peer, dp),
            device_id_type=MESH,
        )

    def hand_back(k):
        peer = lax.rem(ep + k + 1, n_ep)
        return pltpu.make_async_remote_copy(
            src_ref=cbuf.at[peer],
            dst_ref=grad_out.at[ep],
            send_sem=csend.at[k],
            recv_sem=crecv.at[k],
            device_id=(peer, dp),
            device_id_type=MESH,
        )

    def home(t, k):
        peer = lax.rem(ep + k + 1, n_ep)
        return pltpu.make_async_remote_copy(
            src_ref=part.at[lax.rem(dp + t, n_dp), peer, :, rest],
            dst_ref=back.at[t, ep, :, rest],
            send_sem=bsend.at[t, k],
            recv_sem=brecv.at[t, k],
            device_id=(peer, dp),
            device_id_type=MESH,
        )

    def along(t):
        return pltpu.make_async_remote_copy(
            src_ref=zout.at[t - 1],
            dst_ref=zin.at[t - 1],
            send_sem=zsend.at[t - 1],
            recv_sem=zrecv.at[t - 1],
            device_id=(ep, lax.rem(dp + t, n_dp)),
            device_id_type=MESH,
        )

    def share(t):
        target = lax.rem(dp + t, n_dp)
        return pltpu.make_async_remote_copy(
            src_ref=part.at[target, :, :, first],
            dst_ref=shares.at[t - 1],
            send_sem=hsend.at[t - 1],
            recv_sem=hrecv.at[t - 1],
            device_id=(ep, target),
            device_id_type=MESH,
        )

    def bring(k):
        peer = lax.rem(ep + k + 1, n_ep)
        return pltpu.make_async_remote_copy(
            src_ref=mine.at[peer],
            dst_ref=back.at[0, ep, :, first],
            send_sem=msend.at[k],
            recv_sem=mrecv.at[k],
            device_id=(peer, dp),
            device_id_type=MESH,
        )

    def loop(fn):
        def body(k, _):
            fn(k)
            return 0

        lax.fori_loop(0, n_ep - 1, body, 0)

    order = list(range(1, n_dp)) + [0]
    loop(lambda k: give(k).start())
    for t in range(1, n_dp):
        share(t).start()
    for t in order:
        loop(lambda k: home(t, k).start())

    loop(lambda k: give(k).wait_recv())
    gbuf[ep] = pieces[ep]

    def merge(s, _):
        def add(r, acc):
            factor = jnp.where(expert[s] == expert[r], 1.0, 0.0)
            return acc + gbuf[r].astype(jnp.float32) * factor

        acc = lax.fori_loop(0, n_ep, add, jnp.zeros((rows, width), jnp.float32))
        cbuf[s] = acc.astype(jnp.bfloat16)
        return 0

    lax.fori_loop(0, n_ep, merge, 0)
    loop(lambda k: hand_back(k).start())
    own = pltpu.make_async_copy(cbuf.at[ep], grad_out.at[ep], local)
    own.start()

    for t in range(1, n_dp):
        share(t).wait_recv()

    def sum_share(e, _):
        acc = part[dp, e, :, first].astype(jnp.float32)
        for t in range(1, n_dp):
            acc = acc + shares[t - 1, e].astype(jnp.float32)
        mine[e] = acc.astype(jnp.bfloat16)
        return 0

    lax.fori_loop(0, n_ep, sum_share, 0)
    loop(lambda k: bring(k).start())
    back[0, ep, :, first] = mine[ep]

    for t in order:
        loop(lambda k: home(t, k).wait_recv())
        back[t, ep, :, rest] = part[lax.rem(dp + t, n_dp), ep, :, rest]
        if t == 0:
            loop(lambda k: bring(k).wait_recv())
        used = pl.ds(0, pieces.shape[2]) if t == 0 else rest
        total[...] = jnp.zeros_like(total)

        def gather(s, _):
            column = (lax.broadcasted_iota(jnp.int32, (tok, cap), 1) + s * cap).astype(jnp.float32)
            hit = jnp.zeros((tok, cap), jnp.float32)
            for k in range(topk):
                hit = jnp.where(dest[lax.rem(dp + t, n_dp), :, k : k + 1] == column, 1.0, hit)
            total[:, used] += jnp.dot(
                hit.astype(jnp.bfloat16), back[t, s, :, used], preferred_element_type=jnp.float32
            )
            return 0

        lax.fori_loop(0, n_ep, gather, 0)
        if t > 0:
            zout[t - 1] = total[:, rest].astype(jnp.bfloat16)
            along(t).start()

    for t in range(1, n_dp):
        along(t).wait_recv()
        total[:, rest] += zin[t - 1].astype(jnp.float32)
    token_out[...] = total[...].astype(token_out.dtype)

    loop(lambda k: give(k).wait_send())
    loop(lambda k: hand_back(k).wait())
    for t in range(n_dp):
        loop(lambda k: home(t, k).wait_send())
    for t in range(1, n_dp):
        along(t).wait_send()
        share(t).wait_send()
    loop(lambda k: bring(k).wait_send())
    own.wait()


def per_device(
    tokens, cotangent, slot_choice, gate_values, slot_expert, gate_weight, up_weight, down_weight
):
    n_ep, n_dp = lax.axis_size("ep"), lax.axis_size("dp")
    tok, width = tokens.shape
    topk = slot_choice.shape[1]
    cap = max(2, 5 * tok * topk // (4 * n_ep))
    flat_slot = slot_choice.reshape(-1)
    onehot = (flat_slot[:, None] == jnp.arange(n_ep, dtype=jnp.int32)[None, :]).astype(jnp.int32)
    position = jnp.sum(jnp.cumsum(onehot, axis=0) * onehot, axis=1) - 1
    dest = (flat_slot * cap + position).reshape(tok, topk)
    lines = -(-2 * topk // 8) * 8
    meta = jnp.concatenate(
        [
            dest.T.astype(jnp.float32),
            gate_values.T,
            jnp.zeros((lines - 2 * topk, tok), jnp.float32),
        ],
        axis=0,
    )
    vmem = pl.BlockSpec(memory_space=pltpu.VMEM)
    anywhere = pl.BlockSpec(memory_space=pl.ANY)
    dma = pltpu.SemaphoreType.DMA
    bf16 = jnp.bfloat16
    early = 3 * width // (14 * 128) * 128
    batch = 4 if cap % 8 == 0 and n_ep % 4 == 0 else 1
    routed = jax.ShapeDtypeStruct((n_dp, n_ep, cap, width), bf16)
    rows_x, rows_g, meta_all = pl.pallas_call(
        functools.partial(dispatch_kernel, n_ep, n_dp, cap, topk, early, batch),
        out_shape=(routed, routed, jax.ShapeDtypeStruct((n_dp, lines, tok), jnp.float32)),
        in_specs=[vmem] * 3,
        out_specs=(anywhere, anywhere, vmem),
        scratch_shapes=[
            pltpu.VMEM((n_dp, tok, width - early), bf16),
            pltpu.VMEM((n_dp, tok, width - early), bf16),
            pltpu.VMEM((n_dp, lines, tok), jnp.float32),
            pltpu.VMEM((n_ep, cap, width), bf16),
            pltpu.VMEM((n_ep, cap, width), bf16),
            pltpu.VMEM((n_dp - 1, n_ep, cap, width - early), bf16),
            pltpu.VMEM((n_dp - 1, n_ep, cap, width - early), bf16),
            dma((n_dp, 3, 2)),
            dma((n_dp, 3)),
            dma((n_dp, 2, 2)),
            dma((n_dp, 2)),
            dma((2, n_dp, n_ep)),
            dma((2, n_dp, n_ep)),
            dma((2, n_dp)),
        ],
        compiler_params=pltpu.CompilerParams(
            collective_id=0, has_side_effects=True, vmem_limit_bytes=VMEM_LIMIT
        ),
        name="dispatch",
    )(tokens, cotangent, meta)

    rows_x = rows_x.reshape(-1, width)
    rows_g = rows_g.reshape(-1, width)
    w_gate, w_up, w_down = gate_weight[0], up_weight[0], down_weight[0]
    gate = jnp.dot(rows_x, w_gate, preferred_element_type=jnp.float32)
    up = jnp.dot(rows_x, w_up, preferred_element_type=jnp.float32)
    sig = jax.nn.sigmoid(gate)
    act = (gate * sig * up).astype(bf16)
    d_act = lax.dot_general(
        rows_g, w_down, (((1,), (1,)), ((), ())), preferred_element_type=jnp.float32
    )
    d_gate = (d_act * up * sig * (1.0 + gate * (1.0 - sig))).astype(bf16)
    d_up = (d_act * gate * sig).astype(bf16)
    part = lax.dot_general(
        d_gate, w_gate, (((1,), (1,)), ((), ())), preferred_element_type=jnp.float32
    )
    part = part + lax.dot_general(
        d_up, w_up, (((1,), (1,)), ((), ())), preferred_element_type=jnp.float32
    )
    part = part.astype(bf16).reshape(n_dp, n_ep, cap, width)
    slot_grad = lax.dot_general(
        act, rows_g, (((0,), (0,)), ((), ())), preferred_element_type=jnp.float32
    )
    hidden = slot_grad.shape[0]
    piece = hidden // n_ep
    pieces = slot_grad.astype(bf16).reshape(n_ep, piece, width)

    token_grad, down_grad = pl.pallas_call(
        functools.partial(combine_kernel, n_ep, n_dp, cap, topk, early),
        out_shape=(
            jax.ShapeDtypeStruct((tok, width), bf16),
            jax.ShapeDtypeStruct((n_ep, piece, width), bf16),
        ),
        in_specs=[vmem, vmem, vmem, pl.BlockSpec(memory_space=pltpu.SMEM)],
        out_specs=(vmem, anywhere),
        scratch_shapes=[
            pltpu.VMEM((n_dp, n_ep, cap, width), bf16),
            pltpu.VMEM((n_ep, piece, width), bf16),
            pltpu.VMEM((n_ep, piece, width), bf16),
            pltpu.VMEM((n_dp - 1, tok, width - early), bf16),
            pltpu.VMEM((n_dp - 1, tok, width - early), bf16),
            pltpu.VMEM((tok, width), jnp.float32),
            pltpu.VMEM((n_dp - 1, n_ep, cap, early), bf16),
            pltpu.VMEM((n_ep, cap, early), bf16),
            dma((n_ep,)),
            dma((n_ep,)),
            dma((n_ep,)),
            dma((n_ep,)),
            dma((n_dp, n_ep)),
            dma((n_dp, n_ep)),
            dma((n_dp - 1,)),
            dma((n_dp - 1,)),
            dma((n_dp - 1,)),
            dma((n_dp - 1,)),
            dma((n_ep,)),
            dma((n_ep,)),
            dma,
        ],
        compiler_params=pltpu.CompilerParams(
            collective_id=1, has_side_effects=True, vmem_limit_bytes=VMEM_LIMIT
        ),
        name="combine",
    )(part, pieces, jnp.swapaxes(meta_all[:, :topk, :], 1, 2), slot_expert)
    return token_grad, down_grad.reshape(1, hidden, width)


def solution(mesh):
    return jax.shard_map(
        per_device,
        mesh=mesh,
        in_specs=(
            P(("ep", "dp"), None),
            P(("ep", "dp"), None),
            P(("ep", "dp"), None),
            P(("ep", "dp"), None),
            P(),
            P("ep", None, "dp"),
            P("ep", None, "dp"),
            P("ep", "dp", None),
        ),
        out_specs=(P(("ep", "dp"), None), P("ep", "dp", None)),
        check_vma=False,
    )
```
